32 devices in a mesh: shard: 16 (over z, x, core), task: 2 (over y).
Axes of the slice: x: 2, y: 2, z: 4, core: 2. Of those that a mesh axis runs over, the one named last changes fastest.
Arguments:
- task_deltas: bfloat16 [2, 4, 256, 16384], P('task', None, 'shard')
- rank_scores: int32 [2, 4, 256, 16384], P('task', None, 'shard'), may hold values from 0 to 1073741823
- keep_limits: int32 [2, 4, 8], P('task'), may hold values from 268435456 to 805306367
Outputs:
- merged: bfloat16 [4, 256, 16384], P(None, 'shard', 'task')
The draws below stay inside these ranges and needn't reach their ends.
All inputs are finite; a program needn't handle non-finite values.
Results may differ from the reference program's by a relative error of at most 0.0051.
Values may be sent and summed in bfloat16 or wider, within the bound.
A program may use at most 64 MiB of HBM per device.

```python
import math
import jax
import jax.numpy as jnp
from jax import lax

EXPERTS = 8
FF = 16384
LAYERS = 4
ROWS = 32
TASKS = 2


def draw_task_deltas(key, part):
    key_base, key_column, key_row = jax.random.split(key, 3)
    row_total = EXPERTS * ROWS
    shape = (TASKS, LAYERS, row_total, FF)
    rising = 1.0 + 2.0 * jnp.arange(row_total, dtype=jnp.float32) / max(row_total - 1, 1)
    base = jax.random.normal(key_base, shape, jnp.float32)
    column = 0.03 * jnp.exp(jax.random.uniform(key_column, (TASKS, LAYERS, 1, FF), jnp.float32, 0.0, math.log(10.0)))
    row_scale = jnp.exp(jax.random.uniform(key_row, (TASKS, LAYERS, row_total, 1), jnp.float32, 0.0, math.log(10.0)))
    return (base * column * row_scale * rising[None, None, :, None]).astype(jnp.bfloat16)


def plant(result, stream_key, smallest, top_value):
    longest = result.shape.index(max(result.shape))
    spots = []
    for shift in (0, 1):
        where = [jax.random.randint(jax.random.fold_in(stream_key, axis), (), 0, length) for axis, length in enumerate(result.shape)]
        where[longest] = (where[longest] + shift) % result.shape[longest]
        spots.append(tuple(where))
    return result.at[spots[0]].set(smallest).at[spots[1]].set(top_value)


def setup_inputs(seed: int = 0) -> dict:
    key_list = jax.random.split(jax.random.key(seed), 4)
    return {
        "task_deltas": draw_task_deltas(jax.random.fold_in(key_list[3], 71), 0),
        "rank_scores": plant(jax.random.randint(key_list[1], (TASKS, LAYERS, EXPERTS * ROWS, FF), 0, 1073741824), jax.random.fold_in(key_list[1], 1), 0, 1073741823).astype(jnp.int32),
        "keep_limits": plant(jax.random.randint(key_list[2], (TASKS, LAYERS, EXPERTS), 268435456, 805306368), jax.random.fold_in(key_list[2], 1), 268435456, 805306367).astype(jnp.int32),
    }


def keep_probability(column_sums, grand_sums, row_total):
    column_mean = column_sums / row_total
    grand_mean = grand_sums / (EXPERTS * row_total * FF)
    return (0.2 + 0.7 * column_mean / (column_mean + grand_mean)).astype(jnp.bfloat16)


def reference(task_deltas, rank_scores, keep_limits):
    outputs = []
    for layer_at in range(LAYERS):
        change = task_deltas[:, layer_at].astype(jnp.float32).reshape(TASKS, EXPERTS, ROWS, FF)
        column_sums = jnp.sum(jnp.abs(change), axis=2)
        grand_sums = jnp.sum(column_sums, axis=(1, 2))
        rounded = lax.optimization_barrier(keep_probability(column_sums, grand_sums[:, None, None], ROWS))
        probability = rounded.astype(jnp.float32)
        scores = rank_scores[:, layer_at].reshape(TASKS, EXPERTS, ROWS, FF)
        limits = keep_limits[:, layer_at][:, :, None, None]
        retained = jnp.where(scores < limits, change / probability[:, :, None, :], jnp.float32(0.0))
        merged = jnp.sum(retained, axis=0).reshape(EXPERTS * ROWS, FF).astype(jnp.bfloat16)
        outputs.append(merged)
    return jnp.stack(outputs)
```

```python
import functools
import jax
import jax.numpy as jnp
from jax import lax
from jax.experimental import pallas as pl
from jax.experimental.pallas import tpu as pltpu
from jax.sharding import PartitionSpec as P

EXPERTS = 8
F32 = jnp.float32
MESH = pl.DeviceIdType.MESH


def kernel(
    sizes, delta_hbm, score_hbm, limit_ref, out_hbm,
    delta, score, outgoing, incoming, sums, sums_in, part, part_in,
    chance, chance_in, own_rate, in_rate, own_kept, merged,
    load_sem, send_sem, recv_sem, sums_sem, part_sem, chance_sem, out_sem,
):
    layers, rows, width, tasks, shards = sizes
    columns = width // tasks
    piece = min(2048, columns)
    pieces = columns // piece
    groups = shards // EXPERTS
    group_bits = groups.bit_length() - 1
    all_bits = shards.bit_length() - 1
    me_shard, me_task = lax.axis_index("shard"), lax.axis_index("task")
    expert = me_shard // groups
    row_total = rows * groups

    def xor_peer(bit):
        stride = 2**bit
        odd = lax.rem(me_shard // stride, 2)
        return me_shard + stride * (1 - 2 * odd)

    def task_peer(k):
        return lax.rem(me_task + k, tasks)

    barrier = pltpu.get_barrier_semaphore()
    for k in range(1, tasks):
        pl.semaphore_signal(barrier, inc=1, device_id={"task": task_peer(k)}, device_id_type=MESH)
    for bit in range(all_bits):
        pl.semaphore_signal(barrier, inc=1, device_id={"shard": xor_peer(bit)}, device_id_type=MESH)

    loads = {}

    def start_load(l, k):
        at = pl.ds(pl.multiple_of(task_peer(k) * columns, 128), columns)
        loads[l, k] = (
            pltpu.make_async_copy(score_hbm.at[0, l, :, at], score.at[l, k], load_sem.at[l, k, 0]),
            pltpu.make_async_copy(delta_hbm.at[0, l, :, at], delta.at[l, k], load_sem.at[l, k, 1]),
        )
        for copy in loads[l, k]:
            copy.start()

    def wait_load(l, k):
        for copy in loads[l, k]:
            copy.wait()

    for l in range(layers):
        for k in range(1, tasks):
            start_load(l, k)
    for l in range(layers):
        start_load(l, 0)

    def at_piece(i):
        return pl.ds(i * piece if isinstance(i, int) else pl.multiple_of(i * piece, 128), piece)

    def masked(l, k, at):
        limit = limit_ref[0, l, expert]
        return jnp.where(score[l, k, :, at] < limit, delta[l, k, :, at].astype(F32), 0.0)

    sends = {}

    def start_send(l, k, i):
        at = at_piece(i)
        copy = pltpu.make_async_remote_copy(
            src_ref=outgoing.at[l, k - 1, :, at],
            dst_ref=incoming.at[l, k - 1, :, at],
            send_sem=send_sem.at[l, k - 1, i],
            recv_sem=recv_sem.at[l, k - 1, i],
            device_id={"task": task_peer(k)},
            device_id_type=MESH,
        )
        copy.start()
        sends[l, k, i] = copy

    ready = []
    entered = False
    for l in range(layers):
        for k in range(1, tasks):
            wait_load(l, k)
            for i in range(pieces):
                at = at_piece(i)
                outgoing[l, k - 1, :, at] = masked(l, k, at).astype(jnp.bfloat16)
                if not entered and ready:
                    pl.semaphore_wait(barrier, tasks - 1 + all_bits)
                    entered = True
                if ready and ready[0][0] < layers - 1:
                    start_send(*ready.pop(0))
                ready.append((l, k, i))

    for k in range(tasks):
        for l in range(layers):
            if k == 0:
                wait_load(l, 0)

            def add_up(i, carry, k=k, l=l):
                at = at_piece(i)
                size = jnp.abs(delta[l, k, :, at].astype(F32))
                sums[k, l : l + 1, at] = jnp.sum(size, axis=0, keepdims=True)
                return carry

            lax.fori_loop(0, pieces, add_up, 0)

    def hold_own(l):
        def body(i, carry):
            at = at_piece(i)
            own_kept[l, :, at] = masked(l, 0, at)
            return carry

        lax.fori_loop(0, pieces, body, 0)

    hold_own(0)
    for bit in range(group_bits):
        copy = pltpu.make_async_remote_copy(
            src_ref=sums, dst_ref=sums_in.at[bit],
            send_sem=sums_sem.at[bit, 0], recv_sem=sums_sem.at[bit, 1],
            device_id={"shard": xor_peer(bit)}, device_id_type=MESH,
        )
        copy.start()
        copy.wait()
        for k in range(tasks):

            def join(i, carry, k=k, bit=bit):
                at = at_piece(i)
                sums[k, :, at] = sums[k, :, at] + sums_in[bit, k, :, at]
                return carry

            lax.fori_loop(0, pieces, join, 0)

    total = jnp.zeros((layers, 128), F32)
    for k in range(tasks):

        def gather(i, carry, k=k):
            block = sums[k, :, at_piece(i)]
            for j in range(piece // 128):
                carry = carry + block[:, j * 128 : (j + 1) * 128]
            return carry

        total = lax.fori_loop(0, pieces, gather, total)

    for step, bit in enumerate(range(group_bits, all_bits)):
        part[step] = total
        if step + 1 < layers:
            hold_own(step + 1)
        copy = pltpu.make_async_remote_copy(
            src_ref=part.at[step], dst_ref=part_in.at[step],
            send_sem=part_sem.at[step, 0], recv_sem=part_sem.at[step, 1],
            device_id={"shard": xor_peer(bit)}, device_id_type=MESH,
        )
        copy.start()
        copy.wait()
        total = total + part_in[step]
    for l in range(all_bits - group_bits + 1, layers):
        hold_own(l)
    grand_mean = jnp.sum(total, axis=1, keepdims=True) / (EXPERTS * row_total * width)

    for k in list(range(1, tasks)) + [0]:

        def rate(i, carry, k=k):
            at = at_piece(i)
            mean = sums[k, :, at] / row_total
            keep = (0.2 + 0.7 * mean / (mean + grand_mean)).astype(jnp.bfloat16)
            if k:
                chance[k - 1, :, at] = keep
            else:
                own_rate[:, at] = 1.0 / keep.astype(F32)
            return carry

        lax.fori_loop(0, pieces, rate, 0)
    chances = []
    for k in range(1, tasks):
        copy = pltpu.make_async_remote_copy(
            src_ref=chance.at[k - 1], dst_ref=chance_in.at[k - 1],
            send_sem=chance_sem.at[k - 1, 0], recv_sem=chance_sem.at[k - 1, 1],
            device_id={"task": task_peer(k)}, device_id_type=MESH,
        )
        copy.start()
        chances.append(copy)
    while ready:
        start_send(*ready.pop(0))

    for l in range(layers):

        def rescale(i, carry, l=l):
            at = at_piece(i)
            own_kept[l, :, at] = own_kept[l, :, at] * own_rate[l : l + 1, at]
            return carry

        lax.fori_loop(0, pieces, rescale, 0)

    for k in range(1, tasks):
        chances[k - 1].wait()

        def invert(i, carry, k=k):
            at = at_piece(i)
            in_rate[k - 1, :, at] = 1.0 / chance_in[k - 1, :, at].astype(F32)
            return carry

        lax.fori_loop(0, pieces, invert, 0)

    stores = []
    for l in range(layers):
        for i in range(pieces):
            at = at_piece(i)
            value = own_kept[l, :, at]
            for k in range(1, tasks):
                sends[l, k, i].wait()
                value = value + incoming[l, k - 1, :, at].astype(F32) * in_rate[k - 1, l : l + 1, at]
            merged[l, :, at] = value.astype(jnp.bfloat16)
            copy = pltpu.make_async_copy(merged.at[l, :, at], out_hbm.at[l, :, at], out_sem.at[l, i])
            copy.start()
            stores.append(copy)
    for copy in stores:
        copy.wait()


def on_device(task_deltas, rank_scores, keep_limits):
    tasks, shards = lax.axis_size("task"), lax.axis_size("shard")
    _, layers, rows, width = task_deltas.shape
    columns = width // tasks
    pieces = columns // min(2048, columns)
    others = max(tasks - 1, 1)
    groups = shards // EXPERTS
    group_bits = max(groups.bit_length() - 1, 1)
    rest_bits = max(shards.bit_length() - groups.bit_length(), 1)
    half = jnp.bfloat16
    dma = pltpu.SemaphoreType.DMA
    return pl.pallas_call(
        functools.partial(kernel, (layers, rows, width, tasks, shards)),
        out_shape=jax.ShapeDtypeStruct((layers, rows, columns), half),
        in_specs=[
            pl.BlockSpec(memory_space=pl.ANY),
            pl.BlockSpec(memory_space=pl.ANY),
            pl.BlockSpec(memory_space=pltpu.SMEM),
        ],
        out_specs=pl.BlockSpec(memory_space=pl.ANY),
        scratch_shapes=[
            pltpu.VMEM((layers, tasks, rows, columns), half),
            pltpu.VMEM((layers, tasks, rows, columns), jnp.int32),
            pltpu.VMEM((layers, others, rows, columns), half),
            pltpu.VMEM((layers, others, rows, columns), half),
            pltpu.VMEM((tasks, layers, columns), F32),
            pltpu.VMEM((group_bits, tasks, layers, columns), F32),
            pltpu.VMEM((rest_bits, layers, 128), F32),
            pltpu.VMEM((rest_bits, layers, 128), F32),
            pltpu.VMEM((others, layers, columns), half),
            pltpu.VMEM((others, layers, columns), half),
            pltpu.VMEM((layers, columns), F32),
            pltpu.VMEM((others, layers, columns), F32),
            pltpu.VMEM((layers, rows, columns), F32),
            pltpu.VMEM((layers, rows, columns), half),
            dma((layers, tasks, 2)),
            dma((layers, others, pieces)),
            dma((layers, others, pieces)),
            dma((group_bits, 2)),
            dma((rest_bits, 2)),
            dma((others, 2)),
            dma((layers, pieces)),
        ],
        compiler_params=pltpu.CompilerParams(
            collective_id=0, has_side_effects=True, vmem_limit_bytes=60 * 2**20
        ),
        name="merge",
    )(task_deltas, rank_scores, keep_limits)


def solution(mesh):
    return jax.shard_map(
        on_device,
        mesh=mesh,
        in_specs=(
            P("task", None, "shard", None),
            P("task", None, "shard", None),
            P("task", None, None),
        ),
        out_specs=P(None, "shard", "task"),
        check_vma=False,
    )
```

```python
import functools
import jax
import jax.numpy as jnp
from jax import lax
from jax.experimental import pallas as pl
from jax.experimental.pallas import tpu as pltpu
from jax.sharding import PartitionSpec as P

EXPERTS = 8
F32 = jnp.float32
MESH = pl.DeviceIdType.MESH


def kernel(
    sizes, delta_hbm, score_hbm, limit_hbm, merged,
    limit_ref, delta, score, outgoing, incoming, sums, sums_in, part, part_in,
    chance, chance_in, own_rate, in_rate, own_kept,
    limit_sem, load_sem, send_sem, recv_sem, sums_sem, part_sem, chance_sem, share_sem,
):
    layers, rows, width, tasks, shards = sizes
    columns = width // tasks
    piece = min(4096, columns)
    pieces = columns // piece
    groups = shards // EXPERTS
    group_bits = groups.bit_length() - 1
    all_bits = shards.bit_length() - 1
    me_shard, me_task = lax.axis_index("shard"), lax.axis_index("task")
    expert = me_shard // groups
    row_total = rows * groups

    def flipped(index, mask):
        for bit in range(all_bits):
            stride = 2**bit
            if mask & stride:
                index = index + stride * (1 - 2 * lax.rem(index // stride, 2))
        return index

    def xor_peer(bit):
        return flipped(me_shard, 2**bit)

    def task_peer(k):
        return lax.rem(me_task + k, tasks)

    limit_copy = pltpu.make_async_copy(limit_hbm.at[0], limit_ref, limit_sem)
    limit_copy.start()
    barrier = pltpu.get_barrier_semaphore()
    for k in range(1, tasks):
        pl.semaphore_signal(barrier, inc=1, device_id={"task": task_peer(k)}, device_id_type=MESH)
    greeted = list(range(1, groups)) + [2**bit for bit in range(group_bits, all_bits)]
    for mask in greeted:
        pl.semaphore_signal(
            barrier, inc=1, device_id={"shard": flipped(me_shard, mask)}, device_id_type=MESH
        )

    loads = {}

    def start_load(l, k):
        cuts = pieces if l == 0 and k else 1
        length = columns // cuts
        for i in range(cuts):
            here = pl.ds(i * length, length)
            there = pl.ds(pl.multiple_of(task_peer(k) * columns + i * length, 128), length)
            loads[l, k, i] = [
                pltpu.make_async_copy(whole.at[0, l, :, there], held.at[l, k, :, here], load_sem.at[l, k, i, j])
                for j, (whole, held) in enumerate(((score_hbm, score), (delta_hbm, delta)))
            ]
            for copy in loads[l, k, i]:
                copy.start()

    def wait_load(l, k, i):
        for copy in loads.get((l, k, i), ()):
            copy.wait()

    for l in range(layers):
        for k in range(1, tasks):
            start_load(l, k)
    limit_copy.wait()

    def at_piece(i):
        return pl.ds(i * piece if isinstance(i, int) else pl.multiple_of(i * piece, 128), piece)

    def masked(l, k, at):
        limit = limit_ref[l, expert]
        return jnp.where(score[l, k, :, at] < limit, delta[l, k, :, at].astype(F32), 0.0)

    sends = {}

    def start_send(l, k, i):
        at = at_piece(i)
        copy = pltpu.make_async_remote_copy(
            src_ref=outgoing.at[l, k - 1, :, at],
            dst_ref=incoming.at[l, k - 1, :, at],
            send_sem=send_sem.at[l, k - 1, i],
            recv_sem=recv_sem.at[l, k - 1, i],
            device_id={"task": task_peer(k)},
            device_id_type=MESH,
        )
        copy.start()
        sends[l, k, i] = copy

    ready = []
    entered = False
    for l in range(layers):
        for k in range(1, tasks):
            for i in range(pieces):
                wait_load(l, k, i)
                at = at_piece(i)
                outgoing[l, k - 1, :, at] = masked(l, k, at).astype(jnp.bfloat16)
                if not entered and ready:
                    pl.semaphore_wait(barrier, tasks - 1 + len(greeted))
                    entered = True
                    owed = True
                if ready and ready[0][0] < layers - 1:
                    start_send(*ready.pop(0))
                    if owed:
                        owed = False
                        for own in range(layers):
                            start_load(own, 0)
                ready.append((l, k, i))

    for k in range(tasks):
        for l in range(layers):
            if k == 0:
                wait_load(l, 0, 0)

            def add_up(i, carry, k=k, l=l):
                at = at_piece(i)
                size = jnp.abs(delta[l, k, :, at].astype(F32))
                sums[k, l : l + 1, at] = jnp.sum(size, axis=0, keepdims=True)
                return carry

            lax.fori_loop(0, pieces, add_up, 0)

    def hold_own(l):
        def body(i, carry):
            at = at_piece(i)
            own_kept[l, :, at] = masked(l, 0, at)
            return carry

        lax.fori_loop(0, pieces, body, 0)

    hold_own(0)
    for bit in range(group_bits):
        copy = pltpu.make_async_remote_copy(
            src_ref=sums, dst_ref=sums_in.at[bit],
            send_sem=sums_sem.at[bit, 0], recv_sem=sums_sem.at[bit, 1],
            device_id={"shard": xor_peer(bit)}, device_id_type=MESH,
        )
        copy.start()
        copy.wait()
        for k in range(tasks):

            def join(i, carry, k=k, bit=bit):
                at = at_piece(i)
                sums[k, :, at] = sums[k, :, at] + sums_in[bit, k, :, at]
                return carry

            lax.fori_loop(0, pieces, join, 0)

    total = jnp.zeros((layers, 128), F32)
    for k in range(tasks):

        def gather(i, carry, k=k):
            block = sums[k, :, at_piece(i)]
            for j in range(piece // 128):
                carry = carry + block[:, j * 128 : (j + 1) * 128]
            return carry

        total = lax.fori_loop(0, pieces, gather, total)

    for step, bit in enumerate(range(group_bits, all_bits)):
        part[step] = total
        if step + 1 < layers:
            hold_own(step + 1)
        copy = pltpu.make_async_remote_copy(
            src_ref=part.at[step], dst_ref=part_in.at[step],
            send_sem=part_sem.at[step, 0], recv_sem=part_sem.at[step, 1],
            device_id={"shard": xor_peer(bit)}, device_id_type=MESH,
        )
        copy.start()
        copy.wait()
        total = total + part_in[step]
    for l in range(all_bits - group_bits + 1, layers):
        hold_own(l)
    grand_mean = jnp.sum(total, axis=1, keepdims=True) / (EXPERTS * row_total * width)

    for k in list(range(1, tasks)) + [0]:

        def rate(i, carry, k=k):
            at = at_piece(i)
            mean = sums[k, :, at] / row_total
            keep = (0.2 + 0.7 * mean / (mean + grand_mean)).astype(jnp.bfloat16)
            if k:
                chance[k - 1, :, at] = keep
            else:
                own_rate[:, at] = 1.0 / keep.astype(F32)
            return carry

        lax.fori_loop(0, pieces, rate, 0)
    chances = []
    segment = columns // groups
    mine = pl.ds(pl.multiple_of(lax.rem(me_shard, groups) * segment, 128), segment)
    for k in range(1, tasks):
        copy = pltpu.make_async_remote_copy(
            src_ref=chance.at[k - 1, :, mine], dst_ref=chance_in.at[k - 1, :, mine],
            send_sem=chance_sem.at[k - 1, 0], recv_sem=chance_sem.at[k - 1, 1],
            device_id={"task": task_peer(k)}, device_id_type=MESH,
        )
        copy.start()
        chances.append(copy)
    while ready:
        start_send(*ready.pop(0))

    for l in range(layers):

        def rescale(i, carry, l=l):
            at = at_piece(i)
            own_kept[l, :, at] = own_kept[l, :, at] * own_rate[l : l + 1, at]
            return carry

        lax.fori_loop(0, pieces, rescale, 0)

    shares = {}
    for k in range(1, tasks):
        chances[k - 1].wait()
        for mask in range(1, groups):
            copy = pltpu.make_async_remote_copy(
                src_ref=chance_in.at[k - 1, :, mine], dst_ref=chance_in.at[k - 1, :, mine],
                send_sem=share_sem.at[k - 1, mask - 1, 0], recv_sem=share_sem.at[k - 1, mask - 1, 1],
                device_id={"shard": flipped(me_shard, mask)}, device_id_type=MESH,
            )
            copy.start()
            shares[k, mask] = copy
    for k in range(1, tasks):
        for mask in range(1, groups):
            shares[k, mask].wait()

        def invert(i, carry, k=k):
            at = at_piece(i)
            in_rate[k - 1, :, at] = 1.0 / chance_in[k - 1, :, at].astype(F32)
            return carry

        lax.fori_loop(0, pieces, invert, 0)

    for l in range(layers):
        for i in range(pieces):
            at = at_piece(i)
            value = own_kept[l, :, at]
            for k in range(1, tasks):
                sends[l, k, i].wait()
                value = value + incoming[l, k - 1, :, at].astype(F32) * in_rate[k - 1, l : l + 1, at]
            merged[l, :, at] = value.astype(jnp.bfloat16)


def put_out(value, out_hbm, sem):
    copy = pltpu.make_async_copy(value, out_hbm, sem)
    copy.start()
    copy.wait()


def on_device(task_deltas, rank_scores, keep_limits):
    tasks, shards = lax.axis_size("task"), lax.axis_size("shard")
    _, layers, rows, width = task_deltas.shape
    columns = width // tasks
    pieces = columns // min(4096, columns)
    others = max(tasks - 1, 1)
    groups = shards // EXPERTS
    group_bits = max(groups.bit_length() - 1, 1)
    rest_bits = max(shards.bit_length() - groups.bit_length(), 1)
    half = jnp.bfloat16
    dma = pltpu.SemaphoreType.DMA
    keep_limits = pltpu.with_memory_space_constraint(keep_limits, pltpu.HBM)
    result = pl.pallas_call(
        functools.partial(kernel, (layers, rows, width, tasks, shards)),
        out_shape=jax.ShapeDtypeStruct((layers, rows, columns), half),
        in_specs=[
            pl.BlockSpec(memory_space=pltpu.HBM),
            pl.BlockSpec(memory_space=pltpu.HBM),
            pl.BlockSpec(memory_space=pltpu.HBM),
        ],
        out_specs=pl.BlockSpec(memory_space=pltpu.VMEM),
        scratch_shapes=[
            pltpu.SMEM(keep_limits.shape[1:], jnp.int32),
            pltpu.VMEM((layers, tasks, rows, columns), half),
            pltpu.VMEM((layers, tasks, rows, columns), jnp.int32),
            pltpu.VMEM((layers, others, rows, columns), half),
            pltpu.VMEM((layers, others, rows, columns), half),
            pltpu.VMEM((tasks, layers, columns), F32),
            pltpu.VMEM((group_bits, tasks, layers, columns), F32),
            pltpu.VMEM((rest_bits, layers, 128), F32),
            pltpu.VMEM((rest_bits, layers, 128), F32),
            pltpu.VMEM((others, layers, columns), half),
            pltpu.VMEM((others, layers, columns), half),
            pltpu.VMEM((layers, columns), F32),
            pltpu.VMEM((others, layers, columns), F32),
            pltpu.VMEM((layers, rows, columns), F32),
            dma(()),
            dma((layers, tasks, pieces, 2)),
            dma((layers, others, pieces)),
            dma((layers, others, pieces)),
            dma((group_bits, 2)),
            dma((rest_bits, 2)),
            dma((others, 2)),
            dma((others, max(groups - 1, 1), 2)),
        ],
        compiler_params=pltpu.CompilerParams(
            collective_id=0, has_side_effects=True, vmem_limit_bytes=52 * 2**20
        ),
        name="merge",
    )(task_deltas, rank_scores, keep_limits)
    return pl.pallas_call(
        put_out,
        out_shape=jax.ShapeDtypeStruct(result.shape, result.dtype),
        in_specs=[pl.BlockSpec(memory_space=pltpu.VMEM)],
        out_specs=pl.BlockSpec(memory_space=pltpu.HBM),
        scratch_shapes=[dma(())],
        compiler_params=pltpu.CompilerParams(vmem_limit_bytes=4 * 2**20),
        name="put",
    )(result)


def solution(mesh):
    return jax.shard_map(
        on_device,
        mesh=mesh,
        in_specs=(
            P("task", None, "shard", None),
            P("task", None, "shard", None),
            P("task", None, None),
        ),
        out_specs=P(None, "shard", "task"),
        check_vma=False,
    )
```
